32 devices in a mesh: row: 8 (over z, x), col: 4 (over y, core).
Axes of the slice: x: 2, y: 2, z: 4, core: 2. Of those that a mesh axis runs over, the one named last changes fastest.
Arguments:
- tile_values: bfloat16 [192, 512, 128], P('row', 'col'), may hold values from -0.0546875 to 0.0546875
- tile_counts: int32 [96, 4], P('row', 'col'), may hold values from 0 to 2, as said below
- tile_cols: int32 [192, 4], P('row', 'col'), may hold values from 0 to 1, as said below
- panels: bfloat16 [12288, 4096], P('row', 'col'), may hold values from -6 to 6
Outputs:
- product: bfloat16 [1024, 4096], P('col', 'row')
The draws below stay inside these ranges and needn't reach their ends.
Inputs may be any that keep to these rules, and one draw needn't show every extreme that they name: `tile_counts`: within each device the filled slots follow block row order; a device holds at most 24 tiles and some device holds exactly 24 in every draw. `tile_cols`: within one block row of a device the filled slots' columns rise strictly; entries of unfilled slots carry no meaning.
All inputs are finite; a program needn't handle non-finite values.
Results may differ from the reference program's by a relative error of at most 0.001.
Values may be sent and summed in bfloat16 or wider, within the bound.
A program may use at most 64 MiB of HBM per device.

```python
import jax
import jax.numpy as jnp
from jax import lax

TILE = 128
NB = 4096
BR_DEV = 12
BC_DEV = 2
CAP = 24
ROWS = 12288
COLS = 1024
N_ROW = 8
N_COL = 4


def tile_pattern(key):
    base = jax.random.fold_in(key, 7)
    key_levels = jax.random.fold_in(base, 1)
    key_rolled = jax.random.fold_in(base, 2)
    key_chosen = jax.random.fold_in(base, 3)
    levels = jax.random.randint(key_levels, (N_ROW, N_COL, BR_DEV, 1), 0, 5)
    chosen = jax.random.randint(key_chosen, (), 0, N_ROW * N_COL)
    device_ids = jnp.arange(N_ROW, dtype=jnp.int32)[:, None] * N_COL + jnp.arange(N_COL, dtype=jnp.int32)[None, :]
    levels = jnp.where((device_ids == chosen)[:, :, None, None], 4, levels)
    rolled = jax.random.randint(key_rolled, (N_ROW, N_COL, BR_DEV, BC_DEV), 0, 4)
    present = (rolled < levels).astype(jnp.int32)
    counts = jnp.sum(present, axis=-1).astype(jnp.int32)
    row_start = (jnp.cumsum(counts, axis=-1) - counts).astype(jnp.int32)
    within = (jnp.cumsum(present, axis=-1) - present).astype(jnp.int32)
    slot_index = jnp.where(present == 1, row_start[..., None] + within, CAP).astype(jnp.int32)
    col_index = jnp.broadcast_to(jnp.arange(BC_DEV, dtype=jnp.int32), present.shape)

    def place_row(slots, values):
        return jnp.zeros((CAP,), jnp.int32).at[slots].set(values, mode='drop')
    columns = jax.vmap(place_row)(slot_index.reshape(N_ROW * N_COL, BR_DEV * BC_DEV), col_index.reshape(N_ROW * N_COL, BR_DEV * BC_DEV))
    return (counts, columns.reshape(N_ROW, N_COL, CAP))


def draw_tile_counts(key, part):
    counts, columns = tile_pattern(key)
    return jnp.transpose(counts, (0, 2, 1)).reshape(N_ROW * BR_DEV, N_COL)


def draw_tile_cols(key, part):
    counts, columns = tile_pattern(key)
    return jnp.transpose(columns, (0, 2, 1)).reshape(N_ROW * CAP, N_COL)


def strengthened(array, stream_key, source, target, blocks, factor):
    owner, partner = [(jnp.arange(array.shape[dim]) // (array.shape[dim] // blocks)).reshape([-1 if axis == dim else 1 for axis in range(array.ndim)]) for dim in (source, target)]
    chosen = jax.random.permutation(stream_key, blocks)[partner]
    strong = (owner == chosen) | (owner == (partner + blocks // 2) % blocks)
    return jnp.where(strong, factor * array, array)


def block_levels(stream_key, dims, split, smallest, top_value):
    factor_of, own = 1.0, jax.random.fold_in(stream_key, 6)
    for axis_at, blocks in split:
        steps = jnp.exp(jax.random.uniform(jax.random.fold_in(own, axis_at), (blocks,), jnp.float32, smallest / len(split), top_value / len(split)))
        factor_of = factor_of * jnp.repeat(steps, dims[axis_at] // blocks).reshape([-1 if axis == axis_at else 1 for axis in range(len(dims))])
    return factor_of


def centred(stream_key, dims, width, reach, cuts=(), kind=jnp.bfloat16):
    entries = width * jax.random.normal(stream_key, dims, jnp.float32)
    if cuts:
        entries = entries * block_levels(stream_key, dims, cuts, -0.22, 0.18)
    return jnp.clip(entries, -reach, reach).astype(kind)


def noise_with(key, shape, width, reach, shards, heavy, held_as=jnp.bfloat16):
    drawn = width * jax.random.normal(key, shape, jnp.float32)
    if shards:
        drawn = drawn * block_levels(key, shape, shards, -0.22, 0.18)
    return jnp.clip(strengthened(drawn, jax.random.fold_in(key, 3), *heavy), -reach, reach).astype(held_as)


def setup_inputs(seed: int = 0) -> dict:
    key_of = jax.random.split(jax.random.key(seed), 5)
    return {
        "tile_values": centred(key_of[0], (N_ROW * CAP, N_COL * TILE, TILE), (TILE * BR_DEV * N_ROW) ** -0.5, 0.0546875, ((0, 8), (1, 4))),
        "tile_counts": draw_tile_counts(jax.random.fold_in(key_of[4], 71), 0),
        "tile_cols": draw_tile_cols(jax.random.fold_in(key_of[4], 71), 0),
        "panels": noise_with(key_of[3], (ROWS, NB), 1.0, 6.0, ((0, 8), (1, 4)), (0, 1, 8, 2.0)),
    }


def reference(tile_values, tile_counts, tile_cols, panels):
    def add_group(row_dev, totals):
        row_dev = jnp.asarray(row_dev).astype(jnp.int32)
        tile_slab = lax.dynamic_slice_in_dim(tile_values, row_dev * CAP, CAP, 0)
        tile_slab = tile_slab.astype(jnp.float32).reshape(CAP, N_COL, TILE, TILE)
        counts = lax.dynamic_slice_in_dim(tile_counts, row_dev * BR_DEV, BR_DEV, 0).astype(jnp.int32)
        columns = lax.dynamic_slice_in_dim(tile_cols, row_dev * CAP, CAP, 0).astype(jnp.int32)
        row_start = (jnp.cumsum(counts, axis=0) - counts).astype(jnp.int32)
        slot_ids = jnp.arange(CAP, dtype=jnp.int32)[:, None, None]
        row_mask = ((slot_ids >= row_start[None]) & (slot_ids < (row_start + counts)[None])).astype(jnp.float32)
        col_mask = (columns[:, None, :] == jnp.arange(BC_DEV, dtype=jnp.int32)[None, :, None]).astype(jnp.float32)
        dense_rows = jnp.einsum("sic,sjc,scab->iacjb", row_mask, col_mask, tile_slab)
        dense_rows = dense_rows.reshape(BR_DEV * TILE, N_COL * BC_DEV * TILE).astype(jnp.bfloat16)
        panel_rows = lax.dynamic_slice_in_dim(panels, row_dev * BR_DEV * TILE, BR_DEV * TILE, 0)
        return totals + lax.dot_general(dense_rows, panel_rows, (((0,), (0,)), ((), ())), preferred_element_type=jnp.float32)

    totals = lax.fori_loop(0, N_ROW, add_group, jnp.zeros((COLS, NB), jnp.float32))
    return totals.astype(jnp.bfloat16)
```

```python
import functools

import jax
import jax.numpy as jnp
from jax import lax
from jax.experimental import pallas as pl
from jax.experimental.pallas import tpu as pltpu
from jax.sharding import PartitionSpec as P

BC_DEV = 2
PAIR = 2
AHEAD = 4
MESH = pl.DeviceIdType.MESH


def build_dense(counts_ref, cols_ref, tiles_ref, at_ref):
    slots, tile, _ = tiles_ref.shape
    start = jnp.int32(0)
    for i in range(counts_ref.shape[0]):
        count = counts_ref[i, 0]
        here = jnp.minimum(start, slots - 1)
        after = jnp.minimum(start + 1, slots - 1)
        for j in range(BC_DEV):
            one = (count > 0) & (cols_ref[here, 0] == j)
            two = (count > 1) & (cols_ref[after, 0] == j)
            block = tiles_ref[jnp.where(two, after, here)]
            keep = jnp.where(one | two, 1.0, 0.0).astype(jnp.float32)
            block = (block.astype(jnp.float32) * keep).T.astype(jnp.bfloat16)
            at_ref[2 * j, :, i * tile : (i + 1) * tile] = block
        start = start + count


def kernel(
    n_row, n_col, counts_ref, cols_ref, tiles_ref, b_ref, o_ref,
    at_ref, own_ref, xs_ref, xr_ref, zup_ref, zdn_ref, fin_ref, land_ref,
    at_send, at_recv, fw_send, x_send, x_recv, z_send, up_recv, dn_recv, f_send, f_recv,
):
    row, col = lax.axis_index("row"), lax.axis_index("col")
    n_z, n_y = n_row // PAIR, n_col // PAIR
    chunks = 2 * n_col
    z, x = row // PAIR, lax.rem(row, PAIR)
    y, k = col // PAIR, lax.rem(col, PAIR)
    wide = b_ref.shape[1] // PAIR

    def row_of(z_at, x_at):
        return z_at * PAIR + x_at

    def col_of(y_at, k_at):
        return y_at * PAIR + k_at

    beside = (row_of(z, 1 - x), col)
    above = (row_of(lax.rem(z + 1, n_z), x), col)
    below = (row_of(lax.rem(z + n_z - 1, n_z), x), col)
    partner = (row, col_of(y, 1 - k))

    barrier = pltpu.get_barrier_semaphore()
    for other in (beside, above, below):
        pl.semaphore_signal(barrier, inc=1, device_id=other, device_id_type=MESH)
    for step in range(1, n_col):
        pl.semaphore_signal(
            barrier, inc=1, device_id=(row, lax.rem(col + step, n_col)), device_id_type=MESH
        )
    build_dense(counts_ref, cols_ref, tiles_ref, at_ref)
    pl.semaphore_wait(barrier, 3 + n_col - 1)

    def copy(src, dst, send, recv, device):
        return pltpu.make_async_remote_copy(
            src_ref=src, dst_ref=dst, send_sem=send, recv_sem=recv,
            device_id=device, device_id_type=MESH,
        )

    first = []
    for j in range(BC_DEV):
        first.append(copy(at_ref.at[2 * j], at_ref.at[2 * j + 1], at_send.at[j],
                          at_recv.at[2 * j + 1], partner))
        for dy in range(1, n_y):
            to = (row, col_of(lax.rem(y + n_y - dy, n_y), k))
            slot = dy * 4 + 2 * j
            first.append(copy(at_ref.at[2 * j], at_ref.at[slot], at_send.at[dy * 2 + j],
                              at_recv.at[slot], to))
    for c in first:
        c.start()

    def forward(i):
        return copy(at_ref.at[i], at_ref.at[i + 1], fw_send.at[i], at_recv.at[i + 1], partner)

    def x_copy(i):
        return copy(xs_ref.at[i], xr_ref.at[i], x_send.at[i], x_recv.at[i], beside)

    def down_copy(i):
        return copy(own_ref.at[i], zup_ref.at[i], z_send.at[i], up_recv.at[i], below)

    def up_copy(i):
        return copy(own_ref.at[i], zdn_ref.at[i], z_send.at[i], dn_recv.at[i], above)

    def owner(i):
        dy, kk = i // 4, lax.rem(i, 2)
        return (row, col_of(lax.rem(y + dy, n_y), lax.rem(k + kk, PAIR)))

    def fin_copy(i):
        j = lax.rem(i, 4) // 2
        return copy(fin_ref.at[i], land_ref.at[j], f_send.at[i], f_recv.at[j], owner(i))

    def mine(i):
        return (i // 4 == 0) & (lax.rem(i, 2) == 0)

    def compute(i):
        @pl.when(jnp.logical_not(mine(i)))
        def _():
            copy(at_ref.at[i], at_ref.at[i], fw_send.at[i], at_recv.at[i], partner).wait_recv()

        @pl.when((i // 4 > 0) & (lax.rem(i, 2) == 0))
        def _():
            forward(i).start()

        lhs = at_ref[i]
        away = pl.ds(pl.multiple_of((1 - x) * wide, wide), wide)
        xs_ref[i] = jnp.dot(lhs, b_ref[:, away], preferred_element_type=jnp.float32)
        x_copy(i).start()
        here = pl.ds(pl.multiple_of(x * wide, wide), wide)
        own_ref[i] = jnp.dot(lhs, b_ref[:, here], preferred_element_type=jnp.float32)

    final = z == col

    def combine(i):
        x_copy(i).wait_recv()
        own_ref[i] += xr_ref[i]

        @pl.when((z >= col) & (z < n_z - 1))
        def _():
            down_copy(i).wait_recv()
            own_ref[i] += zup_ref[i]

        @pl.when((z <= col) & (z > 0))
        def _():
            up_copy(i).wait_recv()
            own_ref[i] += zdn_ref[i]

        @pl.when(z > col)
        def _():
            down_copy(i).start()

        @pl.when(z < col)
        def _():
            up_copy(i).start()

        @pl.when(final)
        def _():
            fin_ref[i] = own_ref[i].astype(jnp.bfloat16)

            @pl.when(jnp.logical_not(mine(i)))
            def _():
                fin_copy(i).start()

    def lead(i, carry):
        compute(i)
        return carry

    lax.fori_loop(0, AHEAD, lead, 0)

    def main(i, carry):
        combine(i)

        @pl.when(i + AHEAD < chunks)
        def _():
            compute(i + AHEAD)

        return carry

    lax.fori_loop(0, chunks, main, 0)

    rows = land_ref.shape[1]
    for j in range(BC_DEV):
        @pl.when(final)
        def _(j=j):
            o_ref[j * rows : (j + 1) * rows] = fin_ref[2 * j]

        @pl.when(jnp.logical_not(final))
        def _(j=j):
            copy(fin_ref.at[2 * j], land_ref.at[j], f_send.at[2 * j], f_recv.at[j],
                 partner).wait_recv()
            o_ref[j * rows : (j + 1) * rows] = land_ref[j]

    for c in first:
        c.wait_send()

    def drain(i, carry):
        x_copy(i).wait_send()

        @pl.when((i // 4 > 0) & (lax.rem(i, 2) == 0))
        def _():
            forward(i).wait_send()

        @pl.when(jnp.logical_not(final))
        def _():
            down_copy(i).wait_send()

        @pl.when(final & jnp.logical_not(mine(i)))
        def _():
            fin_copy(i).wait_send()

        return carry

    lax.fori_loop(0, chunks, drain, 0)


def per_device(n_row, n_col, tile_values, tile_counts, tile_cols, panels):
    tile = tile_values.shape[1]
    deep, columns = panels.shape
    wide = columns // PAIR
    chunks = BC_DEV * n_col
    f32, bf16 = jnp.float32, jnp.bfloat16
    vmem = pl.BlockSpec(memory_space=pltpu.VMEM)
    smem = pl.BlockSpec(memory_space=pltpu.SMEM)
    dma = pltpu.SemaphoreType.DMA
    return pl.pallas_call(
        functools.partial(kernel, n_row, n_col),
        out_shape=jax.ShapeDtypeStruct((BC_DEV * tile, wide), bf16),
        in_specs=[smem, smem, vmem, vmem],
        out_specs=vmem,
        scratch_shapes=[
            pltpu.VMEM((chunks, tile, deep), bf16),
            pltpu.VMEM((chunks, tile, wide), f32),
            pltpu.VMEM((chunks, tile, wide), f32),
            pltpu.VMEM((chunks, tile, wide), f32),
            pltpu.VMEM((chunks, tile, wide), f32),
            pltpu.VMEM((chunks, tile, wide), f32),
            pltpu.VMEM((chunks, tile, wide), bf16),
            pltpu.VMEM((BC_DEV, tile, wide), bf16),
            dma((n_col,)),
            dma((chunks,)),
            dma((chunks,)),
            dma((chunks,)),
            dma((chunks,)),
            dma((chunks,)),
            dma((chunks,)),
            dma((chunks,)),
            dma((chunks,)),
            dma((BC_DEV,)),
        ],
        compiler_params=pltpu.CompilerParams(
            collective_id=0, has_side_effects=True, vmem_limit_bytes=56 * 1024 * 1024
        ),
    )(tile_counts, tile_cols, tile_values, panels)


def solution(mesh):
    n_row, n_col = mesh.shape["row"], mesh.shape["col"]
    return jax.shard_map(
        functools.partial(per_device, n_row, n_col),
        mesh=mesh,
        in_specs=(P("row", "col", None), P("row", "col"), P("row", "col"), P("row", "col")),
        out_specs=P("col", "row"),
        check_vma=False,
    )
```

```python
import functools

import jax
import jax.numpy as jnp
from jax import lax
from jax.experimental import pallas as pl
from jax.experimental.pallas import tpu as pltpu
from jax.sharding import PartitionSpec as P

BC_DEV = 2
PAIR = 2
BEHIND = 3
TOP = 32767.0
MESH = pl.DeviceIdType.MESH


def encode(value_ref, code_ref, step_ref):
    value = value_ref[...]
    peak = jnp.maximum(jnp.max(jnp.abs(value), axis=0, keepdims=True), 1e-30)
    code_ref[...] = jnp.round(value * (TOP / peak)).astype(jnp.int32).astype(jnp.int16)
    step_ref[...] = peak * (1.0 / TOP)


def decode(code_ref, step_ref):
    return code_ref[...].astype(jnp.int32).astype(jnp.float32) * step_ref[...]


def build_dense(counts_ref, cols_ref, tiles_ref, at_ref):
    slots, tile, _ = tiles_ref.shape
    start = jnp.int32(0)
    for i in range(counts_ref.shape[1]):
        count = counts_ref[0, i]
        here = jnp.minimum(start, slots - 1)
        after = jnp.minimum(start + 1, slots - 1)
        for j in range(BC_DEV):
            one = (count > 0) & (cols_ref[0, here] == j)
            two = (count > 1) & (cols_ref[0, after] == j)
            block = tiles_ref[jnp.where(two, after, here)]
            keep = jnp.where(one | two, 1.0, 0.0).astype(jnp.float32)
            block = (block.astype(jnp.float32) * keep).T.astype(jnp.bfloat16)
            at_ref[2 * j, :, i * tile : (i + 1) * tile] = block
        start = start + count


def kernel(
    n_row, n_col, counts_ref, cols_ref, tiles_ref, b_ref, o_ref,
    at_ref, away_ref, total_ref, own_ref, xs, xr, zs, zup, zdn, fin_ref, land_ref,
    at_send, at_recv, fw_send, x_send, x_recv, z_send, up_recv, dn_recv, f_send, f_recv,
):
    row, col = lax.axis_index("row"), lax.axis_index("col")
    n_z, n_y = n_row // PAIR, n_col // PAIR
    chunks = 2 * n_col
    z, x = row // PAIR, lax.rem(row, PAIR)
    y, k = col // PAIR, lax.rem(col, PAIR)
    wide = b_ref.shape[1] // PAIR

    def row_of(z_at, x_at):
        return z_at * PAIR + x_at

    def col_of(y_at, k_at):
        return y_at * PAIR + k_at

    beside = (row_of(z, 1 - x), col)
    above = (row_of(lax.rem(z + 1, n_z), x), col)
    below = (row_of(lax.rem(z + n_z - 1, n_z), x), col)
    partner = (row, col_of(y, 1 - k))

    barrier = pltpu.get_barrier_semaphore()
    for other in (beside, above, below):
        pl.semaphore_signal(barrier, inc=1, device_id=other, device_id_type=MESH)
    for step in range(1, n_col):
        pl.semaphore_signal(
            barrier, inc=1, device_id=(row, lax.rem(col + step, n_col)), device_id_type=MESH
        )
    build_dense(counts_ref, cols_ref, tiles_ref, at_ref)
    pl.semaphore_wait(barrier, 3 + n_col - 1)

    def copy(src, dst, send, recv, device):
        return pltpu.make_async_remote_copy(
            src_ref=src, dst_ref=dst, send_sem=send, recv_sem=recv,
            device_id=device, device_id_type=MESH,
        )

    first = []
    for j in range(BC_DEV):
        first.append(copy(at_ref.at[2 * j], at_ref.at[2 * j + 1], at_send.at[j],
                          at_recv.at[2 * j + 1], partner))
        for dy in range(1, n_y):
            to = (row, col_of(lax.rem(y + n_y - dy, n_y), k))
            slot = dy * 4 + 2 * j
            first.append(copy(at_ref.at[2 * j], at_ref.at[slot], at_send.at[dy * 2 + j],
                              at_recv.at[slot], to))
    for c in first:
        c.start()

    def forward(i):
        return copy(at_ref.at[i], at_ref.at[i + 1], fw_send.at[i], at_recv.at[i + 1], partner)

    class Both:
        def __init__(self, src, dst, send, recv, i, device):
            self.parts = [
                copy(src[t].at[i], dst[t].at[i], send.at[t, i], recv.at[t, i], device)
                for t in range(2)
            ]

        def start(self):
            for part in self.parts:
                part.start()

        def wait_send(self):
            for part in self.parts:
                part.wait_send()

        def wait_recv(self):
            for part in self.parts:
                part.wait_recv()

    def x_copy(i):
        return Both(xs, xr, x_send, x_recv, i, beside)

    def down_copy(i):
        return Both(zs, zup, z_send, up_recv, i, below)

    def up_copy(i):
        return Both(zs, zdn, z_send, dn_recv, i, above)

    def owner(i):
        dy, kk = i // 4, lax.rem(i, 2)
        return (row, col_of(lax.rem(y + dy, n_y), lax.rem(k + kk, PAIR)))

    def fin_copy(i):
        j = lax.rem(i, 4) // 2
        return copy(fin_ref.at[i], land_ref.at[j], f_send.at[i], f_recv.at[j], owner(i))

    def mine(i):
        return (i // 4 == 0) & (lax.rem(i, 2) == 0)

    def compute(i):
        @pl.when(jnp.logical_not(mine(i)))
        def _():
            copy(at_ref.at[i], at_ref.at[i], fw_send.at[i], at_recv.at[i], partner).wait_recv()

        @pl.when((i // 4 > 0) & (lax.rem(i, 2) == 0))
        def _():
            forward(i).start()

        lhs = at_ref[i]
        away = pl.ds(pl.multiple_of((1 - x) * wide, wide), wide)
        away_ref[...] = jnp.dot(lhs, b_ref[:, away], preferred_element_type=jnp.float32)
        encode(away_ref, xs[0].at[i], xs[1].at[i])
        x_copy(i).start()
        here = pl.ds(pl.multiple_of(x * wide, wide), wide)
        own_ref[i] = jnp.dot(lhs, b_ref[:, here], preferred_element_type=jnp.float32)

    final = z == col

    def combine(i):
        x_copy(i).wait_recv()
        total_ref[...] = own_ref[i] + decode(xr[0].at[i], xr[1].at[i])

        @pl.when((z >= col) & (z < n_z - 1))
        def _():
            down_copy(i).wait_recv()
            total_ref[...] += decode(zup[0].at[i], zup[1].at[i])

        @pl.when((z <= col) & (z > 0))
        def _():
            up_copy(i).wait_recv()
            total_ref[...] += decode(zdn[0].at[i], zdn[1].at[i])

        @pl.when(jnp.logical_not(final))
        def _():
            encode(total_ref, zs[0].at[i], zs[1].at[i])

        @pl.when(z > col)
        def _():
            down_copy(i).start()

        @pl.when(z < col)
        def _():
            up_copy(i).start()

        @pl.when(final)
        def _():
            fin_ref[i] = total_ref[...].astype(jnp.bfloat16)

            @pl.when(jnp.logical_not(mine(i)))
            def _():
                fin_copy(i).start()

    def main(i, carry):
        @pl.when(i < chunks)
        def _():
            compute(i)

        @pl.when(i >= BEHIND)
        def _():
            combine(i - BEHIND)

        return carry

    lax.fori_loop(0, chunks + BEHIND, main, 0)

    rows = land_ref.shape[1]
    for j in range(BC_DEV):
        @pl.when(final)
        def _(j=j):
            o_ref[j * rows : (j + 1) * rows] = fin_ref[2 * j]

        @pl.when(jnp.logical_not(final))
        def _(j=j):
            copy(fin_ref.at[2 * j], land_ref.at[j], f_send.at[2 * j], f_recv.at[j],
                 partner).wait_recv()
            o_ref[j * rows : (j + 1) * rows] = land_ref[j]

    for c in first:
        c.wait_send()

    def drain(i, carry):
        x_copy(i).wait_send()

        @pl.when((i // 4 > 0) & (lax.rem(i, 2) == 0))
        def _():
            forward(i).wait_send()

        @pl.when(jnp.logical_not(final))
        def _():
            down_copy(i).wait_send()

        @pl.when(final & jnp.logical_not(mine(i)))
        def _():
            fin_copy(i).wait_send()

        return carry

    lax.fori_loop(0, chunks, drain, 0)


def per_device(n_row, n_col, tile_values, tile_counts, tile_cols, panels):
    tile = tile_values.shape[1]
    deep, columns = panels.shape
    wide = columns // PAIR
    chunks = BC_DEV * n_col
    f32, bf16 = jnp.float32, jnp.bfloat16
    vmem = pl.BlockSpec(memory_space=pltpu.VMEM)
    smem = pl.BlockSpec(memory_space=pltpu.SMEM)
    dma = pltpu.SemaphoreType.DMA
    coded = (pltpu.VMEM((chunks, tile, wide), jnp.int16), pltpu.VMEM((chunks, 1, wide), f32))
    return pl.pallas_call(
        functools.partial(kernel, n_row, n_col),
        out_shape=jax.ShapeDtypeStruct((BC_DEV * tile, wide), bf16),
        in_specs=[smem, smem, vmem, vmem],
        out_specs=vmem,
        scratch_shapes=[
            pltpu.VMEM((chunks, tile, deep), bf16),
            pltpu.VMEM((tile, wide), f32),
            pltpu.VMEM((tile, wide), f32),
            pltpu.VMEM((chunks, tile, wide), f32),
            coded,
            coded,
            coded,
            coded,
            coded,
            pltpu.VMEM((chunks, tile, wide), bf16),
            pltpu.VMEM((BC_DEV, tile, wide), bf16),
            dma((n_col,)),
            dma((chunks,)),
            dma((chunks,)),
            dma((2, chunks)),
            dma((2, chunks)),
            dma((2, chunks)),
            dma((2, chunks)),
            dma((2, chunks)),
            dma((chunks,)),
            dma((BC_DEV,)),
        ],
        compiler_params=pltpu.CompilerParams(
            collective_id=0, has_side_effects=True, vmem_limit_bytes=56 * 1024 * 1024
        ),
    )(tile_counts.T, tile_cols.T, tile_values, panels)


def solution(mesh):
    n_row, n_col = mesh.shape["row"], mesh.shape["col"]
    return jax.shard_map(
        functools.partial(per_device, n_row, n_col),
        mesh=mesh,
        in_specs=(P("row", "col", None), P("row", "col"), P("row", "col"), P("row", "col")),
        out_specs=P("col", "row"),
        check_vma=False,
    )
```

```python
import functools

import jax
import jax.numpy as jnp
from jax import lax
from jax.experimental import pallas as pl
from jax.experimental.pallas import tpu as pltpu
from jax.sharding import PartitionSpec as P

BC_DEV = 2
PAIR = 2
BEHIND = 2
TOP = 32767.0
MESH = pl.DeviceIdType.MESH


def encode(value_ref, code_ref, step_ref):
    value = value_ref[...]
    peak = jnp.maximum(jnp.max(jnp.abs(value), axis=0, keepdims=True), 1e-30)
    code_ref[...] = jnp.round(value * (TOP / peak)).astype(jnp.int32).astype(jnp.int16)
    step_ref[...] = peak * (1.0 / TOP)


def decode(code_ref, step_ref):
    return code_ref[...].astype(jnp.int32).astype(jnp.float32) * step_ref[...]


def build_dense(counts_ref, cols_ref, tiles_ref, at_ref):
    slots, tile, _ = tiles_ref.shape
    start = jnp.int32(0)
    for i in range(counts_ref.shape[1]):
        count = counts_ref[0, i]
        here = jnp.minimum(start, slots - 1)
        after = jnp.minimum(start + 1, slots - 1)
        for j in range(BC_DEV):
            one = (count > 0) & (cols_ref[0, here] == j)
            two = (count > 1) & (cols_ref[0, after] == j)
            block = tiles_ref[jnp.where(two, after, here)]
            keep = jnp.where(one | two, 1.0, 0.0).astype(jnp.float32)
            block = (block.astype(jnp.float32) * keep).T.astype(jnp.bfloat16)
            at_ref[2 * j, :, i * tile : (i + 1) * tile] = block
        start = start + count


def kernel(
    n_row, n_col, counts_ref, cols_ref, tiles_ref, b_ref, o_ref,
    at_ref, away_ref, total_ref, own_ref, xs, xr, zs, zup, zdn, fin_ref, land_ref,
    at_send, at_recv, fw_send, x_send, x_recv, z_send, up_recv, dn_recv, f_send, f_recv,
):
    row, col = lax.axis_index("row"), lax.axis_index("col")
    n_z, n_y = n_row // PAIR, n_col // PAIR
    chunks = 2 * n_col
    z, x = row // PAIR, lax.rem(row, PAIR)
    y, k = col // PAIR, lax.rem(col, PAIR)
    wide = b_ref.shape[1] // PAIR

    def row_of(z_at, x_at):
        return z_at * PAIR + x_at

    def col_of(y_at, k_at):
        return y_at * PAIR + k_at

    beside = (row_of(z, 1 - x), col)
    above = (row_of(lax.rem(z + 1, n_z), x), col)
    below = (row_of(lax.rem(z + n_z - 1, n_z), x), col)
    partner = (row, col_of(y, 1 - k))

    barrier = pltpu.get_barrier_semaphore()
    for other in (beside, above, below):
        pl.semaphore_signal(barrier, inc=1, device_id=other, device_id_type=MESH)
    for step in range(1, n_col):
        pl.semaphore_signal(
            barrier, inc=1, device_id=(row, lax.rem(col + step, n_col)), device_id_type=MESH
        )
    build_dense(counts_ref, cols_ref, tiles_ref, at_ref)
    pl.semaphore_wait(barrier, 3 + n_col - 1)

    def copy(src, dst, send, recv, device):
        return pltpu.make_async_remote_copy(
            src_ref=src, dst_ref=dst, send_sem=send, recv_sem=recv,
            device_id=device, device_id_type=MESH,
        )

    first = []
    for j in range(BC_DEV):
        first.append(copy(at_ref.at[2 * j], at_ref.at[2 * j + 1], at_send.at[j],
                          at_recv.at[2 * j + 1], partner))
        for dy in range(1, n_y):
            to = (row, col_of(lax.rem(y + n_y - dy, n_y), k))
            slot = dy * 4 + 2 * j
            first.append(copy(at_ref.at[2 * j], at_ref.at[slot], at_send.at[dy * 2 + j],
                              at_recv.at[slot], to))
    for c in first:
        c.start()

    def forward(i):
        return copy(at_ref.at[i], at_ref.at[i + 1], fw_send.at[i], at_recv.at[i + 1], partner)

    class Both:
        def __init__(self, src, dst, send, recv, i, device):
            self.parts = [
                copy(src[t].at[i], dst[t].at[i], send.at[t, i], recv.at[t, i], device)
                for t in range(2)
            ]

        def start(self):
            for part in self.parts:
                part.start()

        def wait_send(self):
            for part in self.parts:
                part.wait_send()

        def wait_recv(self):
            for part in self.parts:
                part.wait_recv()

    def x_copy(i):
        return Both(xs, xr, x_send, x_recv, i, beside)

    def down_copy(i):
        return Both(zs, zup, z_send, up_recv, i, below)

    def up_copy(i):
        return Both(zs, zdn, z_send, dn_recv, i, above)

    def owner(i):
        dy, kk = i // 4, lax.rem(i, 2)
        return (row, col_of(lax.rem(y + dy, n_y), lax.rem(k + kk, PAIR)))

    def fin_copy(i):
        j = lax.rem(i, 4) // 2
        return copy(fin_ref.at[i], land_ref.at[j], f_send.at[i], f_recv.at[j], owner(i))

    def mine(i):
        return (i // 4 == 0) & (lax.rem(i, 2) == 0)

    def compute(i):
        @pl.when(jnp.logical_not(mine(i)))
        def _():
            copy(at_ref.at[i], at_ref.at[i], fw_send.at[i], at_recv.at[i], partner).wait_recv()

        @pl.when((i // 4 > 0) & (lax.rem(i, 2) == 0))
        def _():
            forward(i).start()

        lhs = at_ref[i]
        away = pl.ds(pl.multiple_of((1 - x) * wide, wide), wide)
        away_ref[...] = jnp.dot(lhs, b_ref[:, away], preferred_element_type=jnp.float32)
        encode(away_ref, xs[0].at[i], xs[1].at[i])
        x_copy(i).start()
        here = pl.ds(pl.multiple_of(x * wide, wide), wide)
        own_ref[i] = jnp.dot(lhs, b_ref[:, here], preferred_element_type=jnp.float32)

    final = z == col

    def combine(i):
        x_copy(i).wait_recv()
        total_ref[...] = own_ref[i] + decode(xr[0].at[i], xr[1].at[i])

        @pl.when((z >= col) & (z < n_z - 1))
        def _():
            down_copy(i).wait_recv()
            total_ref[...] += decode(zup[0].at[i], zup[1].at[i])

        @pl.when((z <= col) & (z > 0))
        def _():
            up_copy(i).wait_recv()
            total_ref[...] += decode(zdn[0].at[i], zdn[1].at[i])

        @pl.when(jnp.logical_not(final))
        def _():
            encode(total_ref, zs[0].at[i], zs[1].at[i])

        @pl.when(z > col)
        def _():
            down_copy(i).start()

        @pl.when(z < col)
        def _():
            up_copy(i).start()

        @pl.when(final)
        def _():
            fin_ref[i] = total_ref[...].astype(jnp.bfloat16)

            @pl.when(jnp.logical_not(mine(i)))
            def _():
                fin_copy(i).start()

    def main(i, carry):
        @pl.when(i < chunks)
        def _():
            compute(i)

        @pl.when(i >= BEHIND)
        def _():
            combine(i - BEHIND)

        return carry

    lax.fori_loop(0, chunks + BEHIND, main, 0)

    rows = land_ref.shape[1]
    for j in range(BC_DEV):
        @pl.when(final)
        def _(j=j):
            o_ref[j * rows : (j + 1) * rows] = fin_ref[2 * j]

        @pl.when(jnp.logical_not(final))
        def _(j=j):
            copy(fin_ref.at[2 * j], land_ref.at[j], f_send.at[2 * j], f_recv.at[j],
                 partner).wait_recv()
            o_ref[j * rows : (j + 1) * rows] = land_ref[j]

    for c in first:
        c.wait_send()

    def drain(i, carry):
        x_copy(i).wait_send()

        @pl.when((i // 4 > 0) & (lax.rem(i, 2) == 0))
        def _():
            forward(i).wait_send()

        @pl.when(jnp.logical_not(final))
        def _():
            down_copy(i).wait_send()

        @pl.when(final & jnp.logical_not(mine(i)))
        def _():
            fin_copy(i).wait_send()

        return carry

    lax.fori_loop(0, chunks, drain, 0)


def per_device(n_row, n_col, tile_values, tile_counts, tile_cols, panels):
    tile = tile_values.shape[1]
    deep, columns = panels.shape
    wide = columns // PAIR
    chunks = BC_DEV * n_col
    f32, bf16 = jnp.float32, jnp.bfloat16
    vmem = pl.BlockSpec(memory_space=pltpu.VMEM)
    smem = pl.BlockSpec(memory_space=pltpu.SMEM)
    dma = pltpu.SemaphoreType.DMA
    coded = (pltpu.VMEM((chunks, tile, wide), jnp.int16), pltpu.VMEM((chunks, 1, wide), f32))
    return pl.pallas_call(
        functools.partial(kernel, n_row, n_col),
        out_shape=jax.ShapeDtypeStruct((BC_DEV * tile, wide), bf16),
        in_specs=[smem, smem, vmem, vmem],
        out_specs=vmem,
        scratch_shapes=[
            pltpu.VMEM((chunks, tile, deep), bf16),
            pltpu.VMEM((tile, wide), f32),
            pltpu.VMEM((tile, wide), f32),
            pltpu.VMEM((chunks, tile, wide), f32),
            coded,
            coded,
            coded,
            coded,
            coded,
            pltpu.VMEM((chunks, tile, wide), bf16),
            pltpu.VMEM((BC_DEV, tile, wide), bf16),
            dma((n_col,)),
            dma((chunks,)),
            dma((chunks,)),
            dma((2, chunks)),
            dma((2, chunks)),
            dma((2, chunks)),
            dma((2, chunks)),
            dma((2, chunks)),
            dma((chunks,)),
            dma((BC_DEV,)),
        ],
        compiler_params=pltpu.CompilerParams(
            collective_id=0, has_side_effects=True, vmem_limit_bytes=56 * 1024 * 1024
        ),
    )(tile_counts.T, tile_cols.T, tile_values, panels)


def solution(mesh):
    n_row, n_col = mesh.shape["row"], mesh.shape["col"]
    return jax.shard_map(
        functools.partial(per_device, n_row, n_col),
        mesh=mesh,
        in_specs=(P("row", "col", None), P("row", "col"), P("row", "col"), P("row", "col")),
        out_specs=P("col", "row"),
        check_vma=False,
    )
```
